512 devices in a mesh: groups: 2 (over y), rows: 32 (over z), keys: 4 (over x), heads: 2 (over core).
Axes of the slice: x: 4, y: 2, z: 32, core: 2. Of those that a mesh axis runs over, the one named last changes fastest.
The devices are a block of a 4x8x32 slice.
Arguments:
- pair: bfloat16 [2048, 1024, 128], P(('groups', 'rows'), 'keys'), parts along dimension 0, may hold values from -6 to 6
- seq_length: int32 [2], P('groups'), parts along dimension 0, may hold values from 513 to 1024
- tile_counts: int32 [2048, 8], P(('groups', 'rows')), parts along dimension 0, may hold values from 0 to 128, as said below
- ln_gain: float32 [128], replicated, may hold values from 0.5 to 1.5
- w_query: bfloat16 [128, 128], P(None, 'heads'), may hold values from -8 to 8
- w_key: bfloat16 [128, 128], P(None, 'heads'), may hold values from -0.5 to 0.5
- w_value: bfloat16 [128, 128], P(None, 'heads'), may hold values from -0.5 to 0.5
- w_gate: bfloat16 [128, 128], P(None, 'heads'), may hold values from -0.5 to 0.5
- w_bias: bfloat16 [128, 4], P(None, 'heads'), may hold values from -1.5 to 1.5
- w_out: bfloat16 [128, 128], replicated, may hold values from -2 to 2
Outputs:
- update: bfloat16 [2048, 1024, 128], P(('groups', 'rows'), ('keys', 'heads')), parts along dimension 0
The draws below stay inside these ranges and needn't reach their ends.
There are 2 independent parts, one for each index of `groups`. The reference program is written for one: setup_inputs(seed, part) draws one part's arguments, and reference() takes and returns one part's arrays. A program takes and returns all parts, laid end to end along the dimension named above; an argument that names none is the same for every part. Nothing has to cross between parts.
Inputs may be any that keep to these rules, and one draw needn't show every extreme that they name: `tile_counts`: for each row and each tile of 128 keys, how many of the tile's leading keys are valid; some rows have no valid key at all.
All inputs are finite; a program needn't handle non-finite values.
Results may differ from the reference program's by a relative error of at most 0.03.
The reference program's roundings to bfloat16 on the way count: a program that leaves them out, or rounds other values in their place, can miss the bound.
Values may be sent and summed in bfloat16 or wider, within the bound.
No kernel may reach another device: no remote copies, remote signals or barrier semaphores. Data moves between devices by JAX's collectives and lax.ppermute only.
A program may use at most 128 MiB of HBM per device.

```python
import jax
import jax.numpy as jnp
from jax import lax

C = 128
HEADS = 4
HEAD_DIM = 32
TILE = 128
L = 1024


def draw_tile_counts(key, part):
    first, second = jax.random.split(jax.random.fold_in(key, 11))
    counts = jax.random.randint(first, (L, L // TILE), 0, TILE + 1)
    keeper = jax.random.randint(second, (L, 1), 0, 8) > 0
    return jnp.where(keeper, counts, 0).astype(jnp.int32)


def draw_w_query(key, part):
    inner = jax.random.fold_in(key, 23)
    drawn = jnp.clip(jax.random.normal(inner, (C, HEADS * HEAD_DIM), jnp.float32), -4.0, 4.0) * C ** (-0.5)
    return drawn.astype(jnp.bfloat16)


def block_levels(stream_key, extent, cuts, least, top_value):
    def one(position, blocks):
        heights = jax.random.uniform(jax.random.fold_in(jax.random.fold_in(stream_key, 6), position), (blocks,), jnp.float32, least / len(cuts), top_value / len(cuts))
        return jnp.repeat(jnp.exp(heights), extent[position] // blocks).reshape((-1,) + (1,) * (len(extent) - position - 1))

    level = one(*cuts[0])
    for cut in cuts[1:]:
        level = level * one(*cut)
    return level


def centred(rng, extent, deviation, reach, cuts=(), kind=jnp.bfloat16):
    values = deviation * jax.random.normal(rng, extent, jnp.float32)
    if cuts:
        values = values * block_levels(rng, extent, cuts, -0.22, 0.18)
    return jnp.clip(values, -reach, reach).astype(kind)


def setup_inputs(seed: int = 0, part: int = 0) -> dict:
    streams_of = jax.random.split(jax.random.key(seed), 11)
    part_splits = jax.random.split(jax.random.fold_in(streams_of[10], part), 11)
    pair = centred(part_splits[0], (L, L, C), 1.0, 6.0, ((0, 32), (1, 4)))
    seq_length = jax.random.randint(part_splits[1], (1,), L // 2 + 1, L + 1).astype(jnp.int32)
    tile_counts = draw_tile_counts(jax.random.fold_in(jax.random.fold_in(streams_of[10], part), 71), part)
    ln_gain = jnp.clip(1.0 + 0.1 * jax.random.normal(streams_of[3], (C,), jnp.float32), 0.5, 1.5)
    w_query = draw_w_query(jax.random.fold_in(streams_of[10], 71), part)
    w_key = centred(streams_of[5], (C, HEADS * HEAD_DIM), C ** -0.5, 0.5, ((1, 2),))
    w_value = centred(streams_of[6], (C, HEADS * HEAD_DIM), C ** -0.5, 0.5, ((1, 2),))
    w_gate = centred(streams_of[7], (C, HEADS * HEAD_DIM), C ** -0.5, 0.5, ((1, 2),))
    w_bias = centred(streams_of[8], (C, HEADS), (C // 8) ** -0.5, 1.5, ((1, 2),))
    w_out = centred(streams_of[9], (HEADS * HEAD_DIM, C), (HEADS * HEAD_DIM // 16) ** -0.5, 2.0)
    return dict(pair=pair, seq_length=seq_length, tile_counts=tile_counts, ln_gain=ln_gain, w_query=w_query, w_key=w_key, w_value=w_value, w_gate=w_gate, w_bias=w_bias, w_out=w_out)


norm_epsilon = 1e-05
masked_score = -1e+30

def layer_norm(values, gain):
    center = values - lax.optimization_barrier(jnp.mean(values, axis=-1, keepdims=True))
    spread = lax.optimization_barrier(jnp.mean(center * center, axis=-1, keepdims=True))
    return center * lax.rsqrt(spread + norm_epsilon) * gain

def reference(pair, seq_length, tile_counts, ln_gain, w_query, w_key, w_value, w_gate, w_bias, w_out):
    width = HEADS * HEAD_DIM
    normed = layer_norm(pair.astype(jnp.float32), ln_gain).astype(jnp.bfloat16)
    flat = normed.reshape(L * L, C)
    queries = (jnp.dot(flat, w_query, preferred_element_type=jnp.float32) * HEAD_DIM ** (-0.5)).astype(jnp.bfloat16).reshape(L, L, HEADS, HEAD_DIM)
    keys_all = jnp.dot(flat, w_key, preferred_element_type=jnp.float32).astype(jnp.bfloat16).reshape(L, L, HEADS, HEAD_DIM)
    values_all = jnp.dot(flat, w_value, preferred_element_type=jnp.float32).astype(jnp.bfloat16).reshape(L, L, HEADS, HEAD_DIM)
    gate_act = jax.nn.sigmoid(jnp.dot(flat, w_gate, preferred_element_type=jnp.float32)).reshape(L, L, width)
    pair_bias = jnp.einsum('jkc,ch->hjk', normed.astype(jnp.float32), w_bias.astype(jnp.float32))
    positions = jnp.arange(L, dtype=jnp.int32)
    allowed = (positions[None, :] < seq_length[0]) & ((positions % TILE)[None, :] < jnp.repeat(tile_counts, TILE, axis=1))

    def one_row(operands):
        row_queries, row_keys, row_values, row_allowed = operands
        shown = row_allowed[None, None, :]
        scores = jnp.einsum('jhd,khd->hjk', row_queries.astype(jnp.float32), row_keys.astype(jnp.float32)) + pair_bias
        scores = jnp.where(shown, scores, masked_score)
        row_max = lax.optimization_barrier(jnp.max(scores, axis=-1, keepdims=True))
        weights = jnp.where(shown, jnp.exp(scores - row_max), 0.0)
        row_sum = lax.optimization_barrier(jnp.sum(weights, axis=-1))
        rounded = lax.optimization_barrier(weights.astype(jnp.bfloat16)).astype(jnp.float32)
        mixed = jnp.einsum('hjk,khd->jhd', rounded, row_values.astype(jnp.float32))
        denom = jnp.maximum(row_sum, 1.0)
        return (mixed / jnp.transpose(denom)[:, :, None]).astype(jnp.bfloat16)
    attended = lax.map(one_row, (queries, keys_all, values_all, allowed))
    attended = lax.optimization_barrier(attended.reshape(L, L, width)).astype(jnp.float32)
    gated = (gate_act * attended).astype(jnp.bfloat16)
    update = jnp.dot(gated.reshape(L * L, width), w_out, preferred_element_type=jnp.float32)
    return update.astype(jnp.bfloat16).reshape(L, L, C)
```

```python
import functools

import jax
import jax.numpy as jnp
from jax import lax
from jax.experimental import pallas as pl
from jax.experimental.pallas import tpu as pltpu
from jax.sharding import PartitionSpec as P

HEAD_DIM = 32
TILE = 128
NORM_EPSILON = 1e-05
MASKED = -1e30
FLOOR = -1e29
SEGMENT = 8
VMEM_LIMIT = 60 * 1024 * 1024


def shift(size, by):
    return [(i, (i + by) % size) for i in range(size)]


def contract_lanes(a, b):
    return lax.dot_general(a, b, (((1,), (1,)), ((), ())), preferred_element_type=jnp.float32)


def norm_kernel(scalars, pair_ref, gain_ref, wb_ref, half_ref, bias_ref, bias_scr, *, rows):
    half = rows // 2
    core = scalars[0]
    gain = gain_ref[...]
    ones = jnp.full((128, 128), 1.0 / 128, jnp.bfloat16)
    wb = wb_ref[...]

    def normed_row(i):
        raw = pair_ref[i]
        mean = jnp.dot(raw, ones, preferred_element_type=jnp.float32)
        center = raw.astype(jnp.float32) - mean
        spread = jnp.mean(center * center, axis=-1, keepdims=True)
        return (center * lax.rsqrt(spread + NORM_EPSILON) * gain).astype(jnp.bfloat16)

    def one(i, r, keep):
        normed = normed_row(i)
        if keep:
            half_ref[r] = normed
        b = contract_lanes(wb, normed)
        bias_scr[0, pl.ds(i, 1), :] = b[0:1]
        bias_scr[1, pl.ds(i, 1), :] = b[1:2]

    def step(r, carry):
        one(core * half + r, r, True)
        one((1 - core) * half + r, r, False)
        return carry

    lax.fori_loop(0, half, step, 0, unroll=2)
    bias_ref[...] = bias_scr[...].astype(jnp.bfloat16)


def project_kernel(n0, n1, n2, n3a, n3b, wqg, wkv, q_ref, k_ref, v_ref, g_ref, *, half):
    row = pl.program_id(0)
    cols = n0.shape[1]
    w = wkv[...]
    own = n0[0]
    qg = jnp.dot(own, wqg[...], preferred_element_type=jnp.float32)
    q_ref[0] = (qg[:, :128] * HEAD_DIM**-0.5).astype(jnp.bfloat16)
    g_ref[0] = jax.nn.sigmoid(qg[:, 128:])

    def put(block, at):
        kv = jnp.dot(block, w, preferred_element_type=jnp.float32).astype(jnp.bfloat16)
        k_ref[0, at * cols : (at + 1) * cols, :] = kv[:, :128]
        v_ref[0, at * cols : (at + 1) * cols, :] = kv[:, 128:]

    put(own, 0)
    put(n1[0], 1)
    put(n2[0], 2)

    @pl.when(row < half)
    def _():
        put(n3a[0], 3)

    @pl.when(row >= half)
    def _():
        put(n3b[0], 3)


def attend_kernel(scalars, counts, q_ref, k_ref, v_ref, g_ref, b0, b1, b2, *rest, phase, groups):
    if phase == 0:
        out_ref, bias_scr = rest
    else:
        before_ref, wout_ref, out_ref, bias_scr = rest
    row = pl.program_id(0)
    place, lane_at, seq, core = scalars[0], scalars[1], scalars[2], scalars[3]
    cols = q_ref.shape[1]
    block = cols // SEGMENT
    offsets = (0, groups - 1, 1, 2)

    @pl.when(row == 0)
    def _():
        for ref, ds in ((b0, (0, 5, 3)), (b1, (7, 4, 2)), (b2, (1, 6))):
            for n, d in enumerate(ds):
                at = pl.multiple_of(lax.rem(place + d, SEGMENT) * block, block)
                for r in range(groups):
                    who = lax.rem(lane_at + offsets[r], groups)
                    for h in range(2):
                        bias_scr[h, pl.ds(at, block), r * cols : (r + 1) * cols] = ref[
                            n, who, h
                        ].astype(jnp.float32)

    lanes = lax.broadcasted_iota(jnp.int32, (1, TILE), 1)
    shown = []
    per = cols // TILE
    for r in range(groups):
        who = lax.rem(lane_at + offsets[r], groups)
        for t in range(per):
            tile = who * per + t
            limit = jnp.minimum(counts[row * (groups * per) + tile], seq - tile * TILE)
            shown.append(lanes < limit)
    extra = jnp.concatenate([jnp.where(s, 0.0, MASKED) for s in shown], axis=1)
    keys = k_ref[0]
    ones = jnp.ones((keys.shape[0], 128), jnp.bfloat16)
    values = jnp.concatenate([v_ref[0], ones], axis=1)
    q = q_ref[0]
    lane = lax.broadcasted_iota(jnp.int32, (1, 128), 1) // HEAD_DIM
    chunk = 128
    pieces = []
    for at in range(0, cols, chunk):
        total = None
        for h in range(2):
            mine = lane == (2 * phase + h)
            qh = jnp.where(mine, q[at : at + chunk], jnp.zeros_like(q[at : at + chunk]))
            s = contract_lanes(qh, keys) + bias_scr[h, at : at + chunk, :] + extra
            top = jnp.maximum(jnp.max(s, axis=1, keepdims=True), FLOOR)
            p = jnp.exp(s - top).astype(jnp.bfloat16)
            o = jnp.dot(p, values, preferred_element_type=jnp.float32)
            a = o[:, :128] / jnp.maximum(o[:, 128:], 1.0)
            total = jnp.where(mine, a, 0.0 if total is None else total)
        att = total.astype(jnp.bfloat16).astype(jnp.float32)
        gated = (g_ref[0, at : at + chunk, :] * att).astype(jnp.bfloat16)
        if phase == 0:
            out_ref[0, at : at + chunk, :] = gated
        else:
            both = gated + before_ref[0, at : at + chunk, :]
            pieces.append(jnp.dot(both, wout_ref[...], preferred_element_type=jnp.float32))
    if phase == 1:
        update = jnp.concatenate(pieces, axis=0).astype(jnp.bfloat16)
        span = cols // 2
        out_ref[core, 0] = update[:span]
        out_ref[1 - core, 0] = update[span:]


def full(shape):
    return pl.BlockSpec(shape, lambda *_: (0,) * len(shape))


def per_row(shape):
    return pl.BlockSpec((1, *shape), lambda i, *_: (i,) + (0,) * len(shape))


def params():
    return pltpu.CompilerParams(vmem_limit_bytes=VMEM_LIMIT)


def norm(pair, gain, w_bias, core):
    rows, cols, channels = pair.shape
    half = rows // 2
    wb = jnp.zeros((8, channels), jnp.bfloat16).at[: w_bias.shape[1]].set(w_bias.T)
    return pl.pallas_call(
        functools.partial(norm_kernel, rows=rows),
        grid_spec=pltpu.PrefetchScalarGridSpec(
            num_scalar_prefetch=1,
            grid=(1,),
            in_specs=[full(pair.shape), full((1, channels)), full(wb.shape)],
            out_specs=[full((half, cols, channels)), full((2, rows, cols))],
            scratch_shapes=[pltpu.VMEM((2, rows, cols), jnp.float32)],
        ),
        out_shape=[
            jax.ShapeDtypeStruct((half, cols, channels), jnp.bfloat16),
            jax.ShapeDtypeStruct((2, rows, cols), jnp.bfloat16),
        ],
        compiler_params=params(),
        cost_estimate=pl.CostEstimate(
            flops=4_000_000_000, bytes_accessed=4_000_000, transcendentals=0
        ),
        name="norm",
    )(core[None], pair, gain[None], wb)


def project(n0, n1, n2, n3a, n3b, wqg, wkv):
    half, cols, channels = n0.shape
    part = n3a.shape[0]
    groups = 4
    row = per_row((cols, channels))
    wide = per_row((groups * cols, channels))
    first = pl.BlockSpec((1, cols, channels), lambda i: (jnp.minimum(i, part - 1), 0, 0))
    second = pl.BlockSpec((1, cols, channels), lambda i: (jnp.maximum(i - part, 0), 0, 0))
    return pl.pallas_call(
        functools.partial(project_kernel, half=part),
        grid=(half,),
        in_specs=[row, row, row, first, second, full(wqg.shape), full(wkv.shape)],
        out_specs=[row, wide, wide, row],
        out_shape=[
            jax.ShapeDtypeStruct((half, cols, channels), jnp.bfloat16),
            jax.ShapeDtypeStruct((half, groups * cols, channels), jnp.bfloat16),
            jax.ShapeDtypeStruct((half, groups * cols, channels), jnp.bfloat16),
            jax.ShapeDtypeStruct((half, cols, channels), jnp.float32),
        ],
        compiler_params=params(),
        cost_estimate=pl.CostEstimate(
            flops=8_000_000_000, bytes_accessed=16_000_000, transcendentals=0
        ),
        name="project",
    )(n0, n1, n2, n3a, n3b, wqg, wkv)


def attend(scalars, counts, q, k, v, g, blocks, phase, groups, before=None, wout=None):
    half, cols, channels = q.shape
    length = k.shape[1]
    row = per_row((cols, channels))
    wide = per_row((length, channels))
    in_specs = [row, wide, wide, row] + [full(b.shape) for b in blocks]
    args = [q, k, v, g, *blocks]
    if phase == 0:
        out_spec = row
        out_shape = jax.ShapeDtypeStruct((half, cols, channels), jnp.bfloat16)
    else:
        in_specs += [row, full(wout.shape)]
        args += [before, wout]
        out_spec = pl.BlockSpec((2, 1, cols // 2, channels), lambda i, *_: (0, i, 0, 0))
        out_shape = jax.ShapeDtypeStruct((2, half, cols // 2, channels), jnp.bfloat16)
    return pl.pallas_call(
        functools.partial(attend_kernel, phase=phase, groups=groups),
        grid_spec=pltpu.PrefetchScalarGridSpec(
            num_scalar_prefetch=2,
            grid=(half,),
            in_specs=in_specs,
            out_specs=out_spec,
            scratch_shapes=[pltpu.VMEM((2, cols, length), jnp.float32)],
        ),
        out_shape=out_shape,
        compiler_params=params(),
        cost_estimate=pl.CostEstimate(
            flops=14_000_000_000, bytes_accessed=16_000_000, transcendentals=8_000_000
        ),
        name=f"attend{phase}",
    )(scalars, counts, *args)


def per_device(
    pair, seq_length, tile_counts, ln_gain, w_query, w_key, w_value, w_gate, w_bias, w_out
):
    rows, cols, channels = pair.shape
    half = rows // 2
    size = lax.axis_size("rows")
    groups = lax.axis_size("keys")
    core = lax.axis_index("heads")
    place = lax.rem(lax.axis_index("rows"), SEGMENT)
    lane_at = lax.axis_index("keys")
    swap = [(0, 1), (1, 0)]

    mine = jnp.concatenate([w_query, w_key, w_value, w_gate], axis=1)
    other = lax.ppermute(mine, "heads", swap)
    width = w_query.shape[1]

    def joined(n):
        cut = slice(n * width, (n + 1) * width)
        return jnp.concatenate([mine[:, cut], other[:, cut]], axis=1)

    wqg = jnp.concatenate([joined(0), joined(3)], axis=1)
    wkv = jnp.concatenate([joined(1), joined(2)], axis=1)
    wout = jnp.where(core == 0, w_out, jnp.roll(w_out, width, axis=0))

    n0, bias = norm(pair, ln_gain, w_bias, core)

    n1 = lax.ppermute(n0, "keys", shift(groups, 1))
    n2 = lax.ppermute(n0, "keys", shift(groups, -1))

    stride = [[i + SEGMENT * j for j in range(size // SEGMENT)] for i in range(SEGMENT)]
    far = lax.all_gather(bias, "rows", axis=0, axis_index_groups=stride)
    turned = lax.all_to_all(far, "keys", 0, 0, tiled=True)
    down = lax.ppermute(turned, "rows", shift(size, 3))
    up = lax.ppermute(turned, "rows", shift(size, -3))
    three = jnp.stack([turned, down, up])
    below = lax.ppermute(three, "rows", shift(size, 1))
    above = lax.ppermute(three[:2], "rows", shift(size, -1))

    n3a = lax.ppermute(n1[: half // 2], "keys", shift(groups, 1))
    n3b = lax.ppermute(n2[half // 2 :], "keys", shift(groups, -1))
    q, k, v, g = project(n0, n1, n2, n3a, n3b, wqg, wkv)

    blocks = (three, below, above)
    blocks_other = tuple(lax.ppermute(b, "heads", swap) for b in blocks)

    scalars = jnp.stack([place, lane_at, seq_length[0], core]).astype(jnp.int32)
    counts = lax.dynamic_slice_in_dim(tile_counts, core * half, half, 0).reshape(-1)
    gated = attend(scalars, counts, q, k, v, g, blocks, 0, groups)
    update = attend(scalars, counts, q, k, v, g, blocks_other, 1, groups, gated, wout)

    keep, send = update[0], update[1]
    got = lax.ppermute(send, "heads", swap)
    return jnp.where(
        core == 0, jnp.concatenate([keep, got], axis=0), jnp.concatenate([got, keep], axis=0)
    )


def solution(mesh):
    in_specs = (
        P(("groups", "rows"), "keys", None),
        P("groups"),
        P(("groups", "rows"), None),
        P(),
        P(None, "heads"),
        P(None, "heads"),
        P(None, "heads"),
        P(None, "heads"),
        P(None, "heads"),
        P(),
    )
    out_specs = P(("groups", "rows"), ("keys", "heads"), None)
    return jax.shard_map(
        per_device, mesh=mesh, in_specs=in_specs, out_specs=out_specs, check_vma=False
    )
```

```python
import functools

import jax
import jax.numpy as jnp
from jax import lax
from jax.experimental import pallas as pl
from jax.experimental.pallas import tpu as pltpu
from jax.sharding import PartitionSpec as P

HEAD_DIM = 32
TILE = 128
NORM_EPSILON = 1e-05
MASKED = -1e30
FLOOR = -1e29
SEGMENT = 8
STEP = 4
LOG2E = 1.4426950408889634
VMEM_LIMIT = 60 * 1024 * 1024


def shift(size, by):
    return [(i, (i + by) % size) for i in range(size)]


def contract_lanes(a, b):
    return lax.dot_general(a, b, (((1,), (1,)), ((), ())), preferred_element_type=jnp.float32)


def norm_kernel(scalars, pair_ref, gain_ref, wb_ref, half_ref, bias_ref, bias_scr):
    gain = gain_ref[...]
    ones = jnp.full((128, 128), 1.0 / 128, jnp.bfloat16)
    wb = wb_ref[...]
    rows, cols, channels = pair_ref.shape
    group = 4
    for at in range(0, rows, group):
        raw = pair_ref[at : at + group].reshape(group * cols, channels)
        mean = jnp.dot(raw, ones, preferred_element_type=jnp.float32)
        center = raw.astype(jnp.float32) - mean
        spread = jnp.mean(center * center, axis=-1, keepdims=True)
        normed = (center * lax.rsqrt(spread + NORM_EPSILON) * gain).astype(jnp.bfloat16)

        @pl.when(pl.program_id(0) == 0)
        def _():
            half_ref[at : at + group] = normed.reshape(group, cols, channels)

        b = contract_lanes(wb, normed)
        for r in range(group):
            for h in range(2):
                bias_scr[h, at + r : at + r + 1, :] = b[h : h + 1, r * cols : (r + 1) * cols]
    bias_ref[...] = bias_scr[...].astype(jnp.bfloat16)


def project_kernel(n0, n1, n2, n3, wqg, wk, wv, qa, qb, ka, kb, v_ref, g_ref):
    rows, cols, channels = n0.shape
    own = n0[...].reshape(rows * cols, channels)
    qg = jnp.dot(own, wqg[...], preferred_element_type=jnp.float32)
    q = (qg[:, :128] * HEAD_DIM**-0.5).astype(jnp.bfloat16).astype(jnp.float32) * LOG2E
    high = q.astype(jnp.bfloat16)
    low = (q - high.astype(jnp.float32)).astype(jnp.bfloat16)
    shape = (rows, cols, channels)
    qa[...] = jnp.concatenate([high[:, :64], low[:, :64]], axis=1).reshape(shape)
    qb[...] = jnp.concatenate([high[:, 64:], low[:, 64:]], axis=1).reshape(shape)
    g_ref[...] = jax.nn.sigmoid(qg[:, 128:]).reshape(shape)
    for at, ref in enumerate((n0, n1, n2, n3)):
        span = slice(at * cols, (at + 1) * cols)
        block = ref[...].reshape(rows * cols, channels)
        v = jnp.dot(block, wv[...], preferred_element_type=jnp.float32).astype(jnp.bfloat16)
        v_ref[:, span, :] = v.reshape(shape)
        k = contract_lanes(wk[...], block).astype(jnp.bfloat16)
        for r in range(rows):
            ka[r, :, span] = k[:64, r * cols : (r + 1) * cols]
            kb[r, :, span] = k[64:, r * cols : (r + 1) * cols]


def attend_kernel(scalars, counts, q_ref, k_ref, v_ref, g_ref, b0, b1, *rest, phase, groups):
    if phase == 0:
        out_ref, bias_scr, s0, s1, t0, t1 = rest
    else:
        before_ref, wout_ref, keep_ref, send_ref, bias_scr, s0, s1, t0, t1 = rest
    step = pl.program_id(0)
    place, lane_at, seq, core = scalars[0], scalars[1], scalars[2], scalars[3]
    rows, cols, channels = q_ref.shape
    length = cols * groups
    block = cols // SEGMENT
    offsets = (0, groups - 1, 1, 2)

    @pl.when(step == 0)
    def _():
        for ref, ds in ((b0, (0, 5, 3)), (b1, (7, 4, 2, 1, 6))):
            for n, d in enumerate(ds):
                at = pl.multiple_of(lax.rem(place + d, SEGMENT) * block, block)
                for r in range(groups):
                    who = lax.rem(lane_at + offsets[r], groups)
                    for h in range(2):
                        bias_scr[pl.ds(h * cols + at, block), r * cols : (r + 1) * cols] = (
                            ref[n, who, h].astype(jnp.float32) * LOG2E
                        )

    lanes = lax.broadcasted_iota(jnp.int32, (16, TILE), 1)
    per = cols // TILE
    lane = lax.broadcasted_iota(jnp.int32, (1, 128), 1)
    slot = lax.rem(lane, 64) // HEAD_DIM
    one = jnp.where(lane == 0, 1.0, 0.0).astype(jnp.bfloat16)
    flag = jnp.broadcast_to(one, (2 * cols, 128))[:, :16]
    zero = jnp.zeros((cols, 128), jnp.bfloat16)

    def score(i, s_ref, t_ref):
        hide = []
        for r in range(groups):
            who = lax.rem(lane_at + offsets[r], groups)
            for t in range(per):
                tile = who * per + t
                count = counts[(step * rows + i) * (groups * per) + tile]
                limit = jnp.minimum(count, seq - tile * TILE)
                hide.append(jnp.where(lanes < limit, 0.0, MASKED))
        hide = jnp.concatenate(hide, axis=1).astype(jnp.bfloat16)
        k = k_ref[i]
        right = jnp.concatenate([k, k, hide], axis=0)
        q = q_ref[i]
        left = jnp.concatenate([jnp.where(slot == h, q, zero) for h in range(2)], axis=0)
        left = jnp.concatenate([left, flag], axis=1)
        s = jnp.dot(left, right, preferred_element_type=jnp.float32) + bias_scr[...]
        s_ref[...] = s
        top = jnp.maximum(jnp.max(s, axis=1, keepdims=True), FLOOR)
        t_ref[...] = jnp.broadcast_to(top, t_ref.shape)

    def mix(i, s_ref, t_ref):
        values = jnp.concatenate([v_ref[i], jnp.ones((length, 128), jnp.bfloat16)], axis=1)
        p = jnp.concatenate(
            [
                jnp.exp2(s_ref[:, c : c + 128] - t_ref[...]).astype(jnp.bfloat16)
                for c in range(0, length, 128)
            ],
            axis=1,
        )
        o = jnp.dot(p, values, preferred_element_type=jnp.float32)
        a = o[:, :128] / jnp.maximum(o[:, 128:], 1.0)
        first = lane // HEAD_DIM == 2 * phase
        second = lane // HEAD_DIM == 2 * phase + 1
        att = jnp.where(first, a[:cols], jnp.where(second, a[cols:], 0.0))
        att = att.astype(jnp.bfloat16).astype(jnp.float32)
        gated = (g_ref[i] * att).astype(jnp.bfloat16)
        if phase == 0:
            out_ref[i] = gated
        else:
            both = gated + before_ref[i]
            update = jnp.dot(both, wout_ref[...], preferred_element_type=jnp.float32)
            update = update.astype(jnp.bfloat16)
            span = cols // 2
            left, right = update[:span], update[span:]
            keep_ref[i] = jnp.where(core == 0, left, right)
            send_ref[i] = jnp.where(core == 0, right, left)

    bufs = ((s0, t0), (s1, t1))
    score(0, *bufs[0])
    for i in range(rows):
        if i + 1 < rows:
            score(i + 1, *bufs[(i + 1) % 2])
        mix(i, *bufs[i % 2])


def full(shape):
    return pl.BlockSpec(shape, lambda *_: (0,) * len(shape))


def some(rows, shape):
    return pl.BlockSpec((rows, *shape), lambda i, *_: (i,) + (0,) * len(shape))


def params():
    return pltpu.CompilerParams(vmem_limit_bytes=VMEM_LIMIT)


def norm(pair, gain, w_bias, core):
    rows, cols, channels = pair.shape
    half = rows // 2
    return pl.pallas_call(
        norm_kernel,
        grid_spec=pltpu.PrefetchScalarGridSpec(
            num_scalar_prefetch=1,
            grid=(2,),
            in_specs=[
                pl.BlockSpec((half, cols, channels), lambda i, s: (lax.rem(i + s[0], 2), 0, 0)),
                full((1, channels)),
                full((2, channels)),
            ],
            out_specs=[
                full((half, cols, channels)),
                pl.BlockSpec((2, half, cols), lambda i, s: (0, lax.rem(i + s[0], 2), 0)),
            ],
            scratch_shapes=[pltpu.VMEM((2, half, cols), jnp.float32)],
        ),
        out_shape=[
            jax.ShapeDtypeStruct((half, cols, channels), jnp.bfloat16),
            jax.ShapeDtypeStruct((2, rows, cols), jnp.bfloat16),
        ],
        compiler_params=params(),
        cost_estimate=pl.CostEstimate(
            flops=4_000_000_000, bytes_accessed=4_000_000, transcendentals=0
        ),
        name="norm",
    )(core[None], pair, gain[None], w_bias.T)


def project(n0, n1, n2, n3, wqg, wk, wv):
    half, cols, channels = n0.shape
    groups = 4
    length = groups * cols
    step = STEP
    row = some(step, (cols, channels))
    turned = some(step, (64, length))
    shape = jax.ShapeDtypeStruct
    return pl.pallas_call(
        project_kernel,
        grid=(half // step,),
        in_specs=[row, row, row, row, full(wqg.shape), full(wk.shape), full(wv.shape)],
        out_specs=[row, row, turned, turned, some(step, (length, channels)), row],
        out_shape=[
            shape((half, cols, channels), jnp.bfloat16),
            shape((half, cols, channels), jnp.bfloat16),
            shape((half, 64, length), jnp.bfloat16),
            shape((half, 64, length), jnp.bfloat16),
            shape((half, length, channels), jnp.bfloat16),
            shape((half, cols, channels), jnp.float32),
        ],
        compiler_params=params(),
        cost_estimate=pl.CostEstimate(
            flops=8_000_000_000, bytes_accessed=16_000_000, transcendentals=0
        ),
        name="project",
    )(n0, n1, n2, n3, wqg, wk, wv)


def attend(scalars, counts, q, k, v, g, blocks, phase, groups, before=None, wout=None):
    half, cols, channels = q.shape
    length = v.shape[1]
    step = STEP
    row = some(step, (cols, channels))
    in_specs = [row, some(step, (64, length)), some(step, (length, channels)), row]
    in_specs += [full(b.shape) for b in blocks]
    args = [q, k, v, g, *blocks]
    if phase == 0:
        out_specs = row
        out_shape = jax.ShapeDtypeStruct((half, cols, channels), jnp.bfloat16)
    else:
        in_specs += [row, full(wout.shape)]
        args += [before, wout]
        out_specs = [some(step, (cols // 2, channels))] * 2
        out_shape = [jax.ShapeDtypeStruct((half, cols // 2, channels), jnp.bfloat16)] * 2
    return pl.pallas_call(
        functools.partial(attend_kernel, phase=phase, groups=groups),
        grid_spec=pltpu.PrefetchScalarGridSpec(
            num_scalar_prefetch=2,
            grid=(half // step,),
            in_specs=in_specs,
            out_specs=out_specs,
            scratch_shapes=[
                pltpu.VMEM((2 * cols, length), jnp.float32),
                pltpu.VMEM((2 * cols, length), jnp.float32),
                pltpu.VMEM((2 * cols, length), jnp.float32),
                pltpu.VMEM((2 * cols, 128), jnp.float32),
                pltpu.VMEM((2 * cols, 128), jnp.float32),
            ],
        ),
        out_shape=out_shape,
        compiler_params=params(),
        cost_estimate=pl.CostEstimate(
            flops=14_000_000_000, bytes_accessed=16_000_000, transcendentals=8_000_000
        ),
        name=f"attend{phase}",
    )(scalars, counts, *args)


def per_device(
    pair, seq_length, tile_counts, ln_gain, w_query, w_key, w_value, w_gate, w_bias, w_out
):
    rows, cols, channels = pair.shape
    half = rows // 2
    size = lax.axis_size("rows")
    groups = lax.axis_size("keys")
    core = lax.axis_index("heads")
    place = lax.rem(lax.axis_index("rows"), SEGMENT)
    lane_at = lax.axis_index("keys")
    swap = [(0, 1), (1, 0)]

    n0, bias = norm(pair, ln_gain, w_bias, core)

    n1 = lax.ppermute(n0, "keys", shift(groups, 1))
    n2 = lax.ppermute(n0, "keys", shift(groups, -1))
    n3 = lax.ppermute(n0, "keys", shift(groups, 2))

    stride = [[i + SEGMENT * j for j in range(size // SEGMENT)] for i in range(SEGMENT)]
    far = lax.all_gather(bias, "rows", axis=0, axis_index_groups=stride)
    turned = lax.all_to_all(far, "keys", 0, 0, tiled=True)
    down = lax.ppermute(turned, "rows", shift(size, 3))
    up = lax.ppermute(turned, "rows", shift(size, -3))

    mine = jnp.concatenate([w_query, w_key, w_value, w_gate], axis=1)
    mine, _ = lax.optimization_barrier((mine, turned))
    other = lax.ppermute(mine, "heads", swap)
    width = w_query.shape[1]

    def joined(n):
        cut = slice(n * width, (n + 1) * width)
        return jnp.concatenate([mine[:, cut], other[:, cut]], axis=1)

    wqg = jnp.concatenate([joined(0), joined(3)], axis=1)
    wout = jnp.where(core == 0, w_out, jnp.roll(w_out, width, axis=0))
    qa, qb, ka, kb, v, g = project(n0, n1, n2, n3, wqg, joined(1).T, joined(2))
    down, up, qa = lax.optimization_barrier((down, up, qa))

    three = jnp.stack([turned, down, up])
    below = lax.ppermute(three, "rows", shift(size, 1))
    above = lax.ppermute(three[:2], "rows", shift(size, -1))
    five = jnp.concatenate([below, above])

    blocks = (three, five)
    blocks_other = tuple(lax.ppermute(b, "heads", swap) for b in blocks)

    scalars = jnp.stack([place, lane_at, seq_length[0], core]).astype(jnp.int32)
    counts = lax.dynamic_slice_in_dim(tile_counts, core * half, half, 0).reshape(-1)
    gated = attend(scalars, counts, qa, ka, v, g, blocks, 0, groups)
    keep, send = attend(scalars, counts, qb, kb, v, g, blocks_other, 1, groups, gated, wout)

    got = lax.ppermute(send, "heads", swap)
    return jnp.where(
        core == 0, jnp.concatenate([keep, got], axis=0), jnp.concatenate([got, keep], axis=0)
    )


def solution(mesh):
    in_specs = (
        P(("groups", "rows"), "keys", None),
        P("groups"),
        P(("groups", "rows"), None),
        P(),
        P(None, "heads"),
        P(None, "heads"),
        P(None, "heads"),
        P(None, "heads"),
        P(None, "heads"),
        P(),
    )
    out_specs = P(("groups", "rows"), ("keys", "heads"), None)
    return jax.shard_map(
        per_device, mesh=mesh, in_specs=in_specs, out_specs=out_specs, check_vma=False
    )
```

```python
import functools

import jax
import jax.numpy as jnp
from jax import lax
from jax.experimental import pallas as pl
from jax.experimental.pallas import tpu as pltpu
from jax.sharding import PartitionSpec as P


HEAD_DIM = 32
TILE = 128
NORM_EPSILON = 1e-05
MASKED = -1e30
FLOOR = -1e29
SEGMENT = 8
STEP = 8
LOG2E = 1.4426950408889634
NORM_VMEM = 20
PROJECT_VMEM = 20
ATTEND_VMEM = 32


def shift(size, by):
    return [(i, (i + by) % size) for i in range(size)]


def contract_lanes(a, b):
    return lax.dot_general(a, b, (((1,), (1,)), ((), ())), preferred_element_type=jnp.float32)


def norm_kernel(scalars, pair_ref, gain_ref, wb_ref, half_ref, bias_ref, bias_scr):
    gain = gain_ref[...]
    ones = jnp.full((128, 128), 1.0 / 128, jnp.bfloat16)
    wb = wb_ref[...]
    rows, cols, channels = pair_ref.shape
    group = 4
    for at in range(0, rows, group):
        raw = pair_ref[at : at + group].reshape(group * cols, channels)
        mean = jnp.dot(raw, ones, preferred_element_type=jnp.float32)
        center = raw.astype(jnp.float32) - mean
        spread = jnp.mean(center * center, axis=-1, keepdims=True)
        normed = (center * lax.rsqrt(spread + NORM_EPSILON) * gain).astype(jnp.bfloat16)

        @pl.when(pl.program_id(0) == 0)
        def _():
            half_ref[at : at + group] = normed.reshape(group, cols, channels)

        b = contract_lanes(wb, normed)
        for r in range(group):
            for h in range(2):
                bias_scr[h, at + r : at + r + 1, :] = b[h : h + 1, r * cols : (r + 1) * cols]
    bias_ref[...] = bias_scr[...].astype(jnp.bfloat16)


def project_queries(own_ref, pack, q_ref, g_ref):
    rows, cols, channels = own_ref.shape
    own = own_ref[...].reshape(rows * cols, channels)
    qg = jnp.dot(own, pack[:, :256], preferred_element_type=jnp.float32)
    q = (qg[:, :128] * HEAD_DIM**-0.5).astype(jnp.bfloat16).astype(jnp.float32) * LOG2E
    high = q.astype(jnp.bfloat16)
    low = (q - high.astype(jnp.float32)).astype(jnp.bfloat16)
    lane = lax.broadcasted_iota(jnp.int32, (1, 128), 1)
    q_ref[...] = jnp.where(lane < 64, high, low).reshape(own_ref.shape)
    g_ref[...] = jax.nn.sigmoid(qg[:, 128:]).reshape(own_ref.shape)


def project_keys(sources, pack, k_ref, v_ref):
    for at, ref in enumerate(sources):
        rows, cols, channels = ref.shape
        span = slice(at * cols, (at + 1) * cols)
        block = ref[...].reshape(rows * cols, channels)
        v = jnp.dot(block, pack[:, 256:384], preferred_element_type=jnp.float32)
        v_ref[:, span, :] = v.astype(jnp.bfloat16).reshape(ref.shape)
        k = contract_lanes(pack[:64, 384:], block).astype(jnp.bfloat16)
        for r in range(rows):
            k_ref[r, :, span] = k[:, r * cols : (r + 1) * cols]


def project_first(n0, n1, n2, mine, q, g, k, v):
    project_queries(n0, mine, q, g)
    project_keys((n0, n1, n2), mine, k, v)


def project_second(n0, n1, n2, n3, mine, other, q, g, k, v, k_late, v_late):
    project_queries(n0, other, q, g)
    project_keys((n0, n1, n2, n3), other, k, v)
    project_keys((n3,), mine, k_late, v_late)


def attend_kernel(scalars, counts, q_ref, g_ref, *rest, phase, groups):
    parts = 2 - phase
    k_refs, v_refs, rest = rest[:parts], rest[parts : 2 * parts], rest[2 * parts :]
    b0, b1, *rest = rest
    if phase == 0:
        out_ref, bias_scr, s0, s1, t0, t1, done_scr = rest
    else:
        before_ref, wout_ref, keep_ref, send_ref, bias_scr, s0, s1, t0, t1, done_scr = rest
    step = pl.program_id(0)
    place, lane_at, seq, core = scalars[0], scalars[1], scalars[2], scalars[3]
    rows, cols, channels = q_ref.shape
    length = cols * groups
    block = cols // SEGMENT
    offsets = (0, groups - 1, 1, 2)

    @pl.when(step == 0)
    def _():
        for ref, ds in ((b0, (0, 5, 3)), (b1, (7, 4, 2, 1, 6))):
            for n, d in enumerate(ds):
                at = pl.multiple_of(lax.rem(place + d, SEGMENT) * block, block)
                for r in range(groups):
                    who = lax.rem(lane_at + offsets[r], groups)
                    for h in range(2):
                        bias_scr[pl.ds(h * cols + at, block), r * cols : (r + 1) * cols] = (
                            ref[n, who, h].astype(jnp.float32) * LOG2E
                        )

    lanes = lax.broadcasted_iota(jnp.int32, (16, TILE), 1)
    per = cols // TILE
    lane = lax.broadcasted_iota(jnp.int32, (1, 128), 1)
    slot = lax.rem(lane, 64) // HEAD_DIM
    one = jnp.where(lane == 0, 1.0, 0.0).astype(jnp.bfloat16)
    flag = jnp.broadcast_to(one, (2 * cols, 128))[:, :16]
    zero = jnp.zeros((cols, 128), jnp.bfloat16)

    def score(i, s_ref, t_ref):
        hide = []
        for r in range(groups):
            who = lax.rem(lane_at + offsets[r], groups)
            for t in range(per):
                tile = who * per + t
                count = counts[(step * rows + i) * (groups * per) + tile]
                limit = jnp.minimum(count, seq - tile * TILE)
                hide.append(jnp.where(lanes < limit, 0.0, MASKED))
        hide = jnp.concatenate(hide, axis=1).astype(jnp.bfloat16)
        k = jnp.concatenate([ref[i] for ref in k_refs], axis=1)
        right = jnp.concatenate([k, k, hide], axis=0)
        q = q_ref[i]
        left = jnp.concatenate([jnp.where(slot == h, q, zero) for h in range(2)], axis=0)
        left = jnp.concatenate([left, flag], axis=1)
        for c in range(0, length, 256):
            s = jnp.dot(left, right[:, c : c + 256], preferred_element_type=jnp.float32)
            s = s + bias_scr[:, c : c + 256]
            s_ref[:, c : c + 256] = s
            m = jnp.maximum(s[:, :128], s[:, 128:])
            t_ref[...] = m if c == 0 else jnp.maximum(t_ref[...], m)
        top = jnp.maximum(jnp.max(t_ref[...], axis=1, keepdims=True), FLOOR)
        t_ref[...] = jnp.broadcast_to(top, t_ref.shape)

    def mix(i, s_ref, t_ref):
        v = jnp.concatenate([ref[i] for ref in v_refs], axis=0)
        values = jnp.concatenate([v, jnp.ones_like(v)], axis=1)
        p = jnp.concatenate(
            [
                jnp.exp2(s_ref[:, c : c + 128] - t_ref[...]).astype(jnp.bfloat16)
                for c in range(0, length, 128)
            ],
            axis=1,
        )
        o = jnp.dot(p, values, preferred_element_type=jnp.float32)
        a = o[:, :128] / jnp.maximum(o[:, 128:], 1.0)
        first = lane // HEAD_DIM == 0
        second = lane // HEAD_DIM == 1
        att = jnp.where(first, a[:cols], jnp.where(second, a[cols:], 0.0))
        att = att.astype(jnp.bfloat16).astype(jnp.float32)
        gated = (g_ref[i] * att).astype(jnp.bfloat16)
        if phase == 0:
            out_ref[i] = gated
        else:
            done_scr[i * cols : (i + 1) * cols] = gated

    if phase == 1:
        wouts = []
        for c in (core, 1 - core):
            part = wout_ref[pl.ds(pl.multiple_of(c * 64, 64), 64), :]
            wouts.append(jnp.concatenate([part, jnp.zeros_like(part)], axis=0))
    bufs = ((s0, t0), (s1, t1))
    score(0, *bufs[0])
    for i in range(rows):
        if i + 1 < rows:
            score(i + 1, *bufs[(i + 1) % 2])
        mix(i, *bufs[i % 2])
    if phase == 1:
        before = before_ref[...].reshape(rows * cols, channels)
        update = jnp.dot(before, wouts[0], preferred_element_type=jnp.float32)
        update += jnp.dot(done_scr[...], wouts[1], preferred_element_type=jnp.float32)
        update = update.astype(jnp.bfloat16).reshape(q_ref.shape)
        span = cols // 2
        left, right = update[:, :span], update[:, span:]
        keep_ref[...] = jnp.where(core == 0, left, right)
        send_ref[...] = jnp.where(core == 0, right, left)


def full(shape):
    return pl.BlockSpec(shape, lambda *_: (0,) * len(shape))


def some(rows, shape):
    return pl.BlockSpec((rows, *shape), lambda i, *_: (i,) + (0,) * len(shape))


def params(mib):
    return pltpu.CompilerParams(vmem_limit_bytes=mib * 1024 * 1024)


def norm(pair, gain, w_bias, core):
    rows, cols, channels = pair.shape
    half = rows // 2
    return pl.pallas_call(
        norm_kernel,
        grid_spec=pltpu.PrefetchScalarGridSpec(
            num_scalar_prefetch=1,
            grid=(2,),
            in_specs=[
                pl.BlockSpec((half, cols, channels), lambda i, s: (lax.rem(i + s[0], 2), 0, 0)),
                full((1, channels)),
                full((2, channels)),
            ],
            out_specs=[
                full((half, cols, channels)),
                pl.BlockSpec((2, half, cols), lambda i, s: (0, lax.rem(i + s[0], 2), 0)),
            ],
            scratch_shapes=[pltpu.VMEM((2, half, cols), jnp.float32)],
        ),
        out_shape=[
            jax.ShapeDtypeStruct((half, cols, channels), jnp.bfloat16),
            jax.ShapeDtypeStruct((2, rows, cols), jnp.bfloat16),
        ],
        compiler_params=params(NORM_VMEM),
        cost_estimate=pl.CostEstimate(
            flops=4_000_000_000, bytes_accessed=4_000_000, transcendentals=0
        ),
        name="norm",
    )(core[None], pair, gain[None], w_bias.T)


def project(sources, packs):
    half, cols, channels = sources[0].shape
    step = STEP
    second = len(packs) == 2
    row = some(step, (cols, channels))
    shape = jax.ShapeDtypeStruct
    out_specs = [row, row]
    out_shape = [
        shape((half, cols, channels), jnp.bfloat16),
        shape((half, cols, channels), jnp.float32),
    ]
    for blocks in (len(sources), 1) if second else (len(sources),):
        length = blocks * cols
        out_specs += [some(step, (64, length)), some(step, (length, channels))]
        out_shape += [
            shape((half, 64, length), jnp.bfloat16),
            shape((half, length, channels), jnp.bfloat16),
        ]
    return pl.pallas_call(
        project_second if second else project_first,
        grid=(half // step,),
        in_specs=[row] * len(sources) + [full(p.shape) for p in packs],
        out_specs=out_specs,
        out_shape=out_shape,
        compiler_params=params(PROJECT_VMEM),
        cost_estimate=pl.CostEstimate(
            flops=4_000_000_000, bytes_accessed=10_000_000, transcendentals=0
        ),
    )(*sources, *packs)


def attend(scalars, counts, q, g, ks, vs, blocks, phase, groups, before=None, wout=None):
    half, cols, channels = q.shape
    length = groups * cols
    step = STEP
    row = some(step, (cols, channels))
    in_specs = [row, row]
    in_specs += [some(step, a.shape[1:]) for a in (*ks, *vs)]
    in_specs += [full(b.shape) for b in blocks]
    args = [q, g, *ks, *vs, *blocks]
    if phase == 0:
        out_specs = row
        out_shape = jax.ShapeDtypeStruct((half, cols, channels), jnp.bfloat16)
    else:
        in_specs += [row, full(wout.shape)]
        args += [before, wout]
        out_specs = [some(step, (cols // 2, channels))] * 2
        out_shape = [jax.ShapeDtypeStruct((half, cols // 2, channels), jnp.bfloat16)] * 2
    return pl.pallas_call(
        functools.partial(attend_kernel, phase=phase, groups=groups),
        grid_spec=pltpu.PrefetchScalarGridSpec(
            num_scalar_prefetch=2,
            grid=(half // step,),
            in_specs=in_specs,
            out_specs=out_specs,
            scratch_shapes=[
                pltpu.VMEM((2 * cols, length), jnp.float32),
                pltpu.VMEM((2 * cols, length), jnp.float32),
                pltpu.VMEM((2 * cols, length), jnp.float32),
                pltpu.VMEM((2 * cols, 128), jnp.float32),
                pltpu.VMEM((2 * cols, 128), jnp.float32),
                pltpu.VMEM((step * cols, channels), jnp.bfloat16),
            ],
        ),
        out_shape=out_shape,
        compiler_params=params(ATTEND_VMEM),
        cost_estimate=pl.CostEstimate(
            flops=14_000_000_000, bytes_accessed=16_000_000, transcendentals=8_000_000
        ),
    )(scalars, counts, *args)


def per_device(
    pair, seq_length, tile_counts, ln_gain, w_query, w_key, w_value, w_gate, w_bias, w_out
):
    rows, _, _ = pair.shape
    half = rows // 2
    size = lax.axis_size("rows")
    groups = lax.axis_size("keys")
    core = lax.axis_index("heads")
    place = lax.rem(lax.axis_index("rows"), SEGMENT)
    lane_at = lax.axis_index("keys")
    swap = [(0, 1), (1, 0)]

    n0, bias = norm(pair, ln_gain, w_bias, core)

    n1 = lax.ppermute(n0, "keys", shift(groups, 1))
    n2 = lax.ppermute(n0, "keys", shift(groups, -1))

    stride = [[i + SEGMENT * j for j in range(size // SEGMENT)] for i in range(SEGMENT)]
    far = lax.all_gather(bias, "rows", axis=0, axis_index_groups=stride)
    turned = lax.all_to_all(far, "keys", 0, 0, tiled=True)
    down = lax.ppermute(turned, "rows", shift(size, 3))
    up = lax.ppermute(turned, "rows", shift(size, -3))

    blank = jnp.zeros_like(w_query)
    turned_key = jnp.concatenate([w_key.T, blank.T], axis=0)
    mine = jnp.concatenate(
        [w_query, w_query, w_gate, blank, w_value, blank, turned_key], axis=1
    )
    mine, _ = lax.optimization_barrier((mine, far))
    other = lax.ppermute(mine, "heads", swap)
    late, _ = lax.optimization_barrier((n0, far))
    n3 = lax.ppermute(late, "keys", shift(groups, 2))

    q0, g0, k0, v0 = project((n0, n1, n2), (mine,))
    down, up, q0 = lax.optimization_barrier((down, up, q0))

    three = jnp.stack([turned, down, up])
    below = lax.ppermute(three, "rows", shift(size, 1))
    above = lax.ppermute(three[:2], "rows", shift(size, -1))
    other, _ = lax.optimization_barrier((other, q0))
    q1, g1, k1, v1, k_late, v_late = project((n0, n1, n2, n3), (mine, other))
    below, above, q1 = lax.optimization_barrier((below, above, q1))
    five = jnp.concatenate([below, above])

    blocks = (three, five)
    three_other = lax.ppermute(three, "heads", swap)
    blocks_other = (three_other, lax.ppermute(five, "heads", swap))

    scalars = jnp.stack([place, lane_at, seq_length[0], core]).astype(jnp.int32)
    counts = lax.dynamic_slice_in_dim(tile_counts, core * half, half, 0).reshape(-1)
    gated = attend(
        scalars, counts, q0, g0, (k0, k_late), (v0, v_late), blocks, 0, groups
    )
    keep, send = attend(
        scalars, counts, q1, g1, (k1,), (v1,), blocks_other, 1, groups, gated, w_out
    )

    got = lax.ppermute(send, "heads", swap)
    return jnp.where(
        core == 0, jnp.concatenate([keep, got], axis=0), jnp.concatenate([got, keep], axis=0)
    )


def solution(mesh):
    in_specs = (
        P(("groups", "rows"), "keys", None),
        P("groups"),
        P(("groups", "rows"), None),
        P(),
        P(None, "heads"),
        P(None, "heads"),
        P(None, "heads"),
        P(None, "heads"),
        P(None, "heads"),
        P(),
    )
    out_specs = P(("groups", "rows"), ("keys", "heads"), None)

    return jax.shard_map(per_device, mesh=mesh, in_specs=in_specs, out_specs=out_specs, check_vma=False)
```

```python
import functools

import jax
import jax.numpy as jnp
from jax import lax
from jax.experimental import pallas as pl
from jax.experimental.pallas import tpu as pltpu
from jax.sharding import PartitionSpec as P


HEAD_DIM = 32
TILE = 128
NORM_EPSILON = 1e-05
MASKED = -1e30
FLOOR = -1e29
SEGMENT = 8
STEP = 8
LOG2E = 1.4426950408889634
NORM_VMEM = 60
PROJECT_VMEM = 20
ATTEND_VMEM = 32


def shift(size, by):
    return [(i, (i + by) % size) for i in range(size)]


def contract_lanes(a, b):
    return lax.dot_general(a, b, (((1,), (1,)), ((), ())), preferred_element_type=jnp.float32)


def norm_kernel(scalars, pair_ref, gain_ref, wb_ref, half_ref, bias_ref, bias_scr):
    gain = gain_ref[...]
    ones = jnp.full((128, 128), 1.0 / 128, jnp.bfloat16)
    wb = wb_ref[...]
    rows, cols, channels = pair_ref.shape
    group = 4
    for at in range(0, rows, group):
        raw = pair_ref[at : at + group].reshape(group * cols, channels)
        mean = jnp.dot(raw, ones, preferred_element_type=jnp.float32)
        center = raw.astype(jnp.float32) - mean
        spread = jnp.mean(center * center, axis=-1, keepdims=True)
        normed = (center * lax.rsqrt(spread + NORM_EPSILON) * gain).astype(jnp.bfloat16)

        @pl.when(pl.program_id(0) == 0)
        def _():
            half_ref[at : at + group] = normed.reshape(group, cols, channels)

        b = contract_lanes(wb, normed)
        for r in range(group):
            for h in range(2):
                bias_scr[h, at + r : at + r + 1, :] = b[h : h + 1, r * cols : (r + 1) * cols]
    bias_ref[...] = bias_scr[...].astype(jnp.bfloat16)


def project_queries(own_ref, pack, q_ref, g_ref):
    rows, cols, channels = own_ref.shape
    own = own_ref[...].reshape(rows * cols, channels)
    qg = jnp.dot(own, pack[:, :256], preferred_element_type=jnp.float32)
    q = (qg[:, :128] * HEAD_DIM**-0.5).astype(jnp.bfloat16).astype(jnp.float32) * LOG2E
    high = q.astype(jnp.bfloat16)
    low = (q - high.astype(jnp.float32)).astype(jnp.bfloat16)
    lane = lax.broadcasted_iota(jnp.int32, (1, 128), 1)
    q_ref[...] = jnp.where(lane < 64, high, low).reshape(own_ref.shape)
    g_ref[...] = jax.nn.sigmoid(qg[:, 128:]).reshape(own_ref.shape)


def project_keys(sources, pack, k_ref, v_ref):
    for at, ref in enumerate(sources):
        rows, cols, channels = ref.shape
        span = slice(at * cols, (at + 1) * cols)
        block = ref[...].reshape(rows * cols, channels)
        v = jnp.dot(block, pack[:, 256:384], preferred_element_type=jnp.float32)
        v_ref[:, span, :] = v.astype(jnp.bfloat16).reshape(ref.shape)
        k = contract_lanes(pack[:64, 384:], block).astype(jnp.bfloat16)
        for r in range(rows):
            k_ref[r, :, span] = k[:, r * cols : (r + 1) * cols]


def project_first(n0, n1, n2, mine, q, g, k, v):
    project_queries(n0, mine, q, g)
    project_keys((n0, n1, n2), mine, k, v)


def project_second(n0, n1, n2, n3, mine, other, q, g, k, v, k_late, v_late):
    project_queries(n0, other, q, g)
    project_keys((n0, n1, n2, n3), other, k, v)
    project_keys((n3,), mine, k_late, v_late)


def attend_kernel(scalars, counts, q_ref, g_ref, *rest, phase, groups):
    parts = 2 - phase
    k_refs, v_refs, rest = rest[:parts], rest[parts : 2 * parts], rest[2 * parts :]
    b0, b1, *rest = rest
    if phase == 0:
        out_ref, bias_scr, s0, s1, t0, t1, done_scr = rest
    else:
        before_ref, wout_ref, keep_ref, send_ref, bias_scr, s0, s1, t0, t1, done_scr = rest
    step = pl.program_id(0)
    place, lane_at, seq, core = scalars[0], scalars[1], scalars[2], scalars[3]
    rows, cols, channels = q_ref.shape
    length = cols * groups
    block = cols // SEGMENT
    offsets = (0, groups - 1, 1, 2)

    @pl.when(step == 0)
    def _():
        for ref, ds in ((b0, (0, 5, 3)), (b1, (7, 4, 2, 1, 6))):
            for n, d in enumerate(ds):
                at = pl.multiple_of(lax.rem(place + d, SEGMENT) * block, block)
                for r in range(groups):
                    who = lax.rem(lane_at + offsets[r], groups)
                    for h in range(2):
                        bias_scr[pl.ds(h * cols + at, block), r * cols : (r + 1) * cols] = (
                            ref[n, who, h].astype(jnp.float32) * LOG2E
                        )

    lanes = lax.broadcasted_iota(jnp.int32, (16, TILE), 1)
    per = cols // TILE
    lane = lax.broadcasted_iota(jnp.int32, (1, 128), 1)
    slot = lax.rem(lane, 64) // HEAD_DIM
    one = jnp.where(lane == 0, 1.0, 0.0).astype(jnp.bfloat16)
    flag = jnp.broadcast_to(one, (2 * cols, 128))[:, :16]
    zero = jnp.zeros((cols, 128), jnp.bfloat16)

    def score(i, s_ref, t_ref):
        hide = []
        for r in range(groups):
            who = lax.rem(lane_at + offsets[r], groups)
            for t in range(per):
                tile = who * per + t
                count = counts[(step * rows + i) * (groups * per) + tile]
                limit = jnp.minimum(count, seq - tile * TILE)
                hide.append(jnp.where(lanes < limit, 0.0, MASKED))
        hide = jnp.concatenate(hide, axis=1).astype(jnp.bfloat16)
        k = jnp.concatenate([ref[i] for ref in k_refs], axis=1)
        right = jnp.concatenate([k, k, hide], axis=0)
        q = q_ref[i]
        left = jnp.concatenate([jnp.where(slot == h, q, zero) for h in range(2)], axis=0)
        left = jnp.concatenate([left, flag], axis=1)
        for c in range(0, length, 256):
            s = jnp.dot(left, right[:, c : c + 256], preferred_element_type=jnp.float32)
            s = s + bias_scr[:, c : c + 256]
            s_ref[:, c : c + 256] = s
            m = jnp.maximum(s[:, :128], s[:, 128:])
            t_ref[...] = m if c == 0 else jnp.maximum(t_ref[...], m)
        top = jnp.maximum(jnp.max(t_ref[...], axis=1, keepdims=True), FLOOR)
        t_ref[...] = jnp.broadcast_to(top, t_ref.shape)

    def mix(i, s_ref, t_ref):
        v = jnp.concatenate([ref[i] for ref in v_refs], axis=0)
        values = jnp.concatenate([v, jnp.ones_like(v)], axis=1)
        p = jnp.concatenate(
            [
                jnp.exp2(s_ref[:, c : c + 128] - t_ref[...]).astype(jnp.bfloat16)
                for c in range(0, length, 128)
            ],
            axis=1,
        )
        o = jnp.dot(p, values, preferred_element_type=jnp.float32)
        a = o[:, :128] / jnp.maximum(o[:, 128:], 1.0)
        first = lane // HEAD_DIM == 0
        second = lane // HEAD_DIM == 1
        att = jnp.where(first, a[:cols], jnp.where(second, a[cols:], 0.0))
        att = att.astype(jnp.bfloat16).astype(jnp.float32)
        gated = (g_ref[i] * att).astype(jnp.bfloat16)
        if phase == 0:
            out_ref[i] = gated
        else:
            done_scr[i * cols : (i + 1) * cols] = gated

    if phase == 1:
        wouts = []
        for c in (core, 1 - core):
            part = wout_ref[pl.ds(pl.multiple_of(c * 64, 64), 64), :]
            wouts.append(jnp.concatenate([part, jnp.zeros_like(part)], axis=0))
    bufs = ((s0, t0), (s1, t1))
    score(0, *bufs[0])
    for i in range(rows):
        if i + 1 < rows:
            score(i + 1, *bufs[(i + 1) % 2])
        mix(i, *bufs[i % 2])
    if phase == 1:
        before = before_ref[...].reshape(rows * cols, channels)
        update = jnp.dot(before, wouts[0], preferred_element_type=jnp.float32)
        update += jnp.dot(done_scr[...], wouts[1], preferred_element_type=jnp.float32)
        update = update.astype(jnp.bfloat16).reshape(q_ref.shape)
        span = cols // 2
        left, right = update[:, :span], update[:, span:]
        keep_ref[...] = jnp.where(core == 0, left, right)
        send_ref[...] = jnp.where(core == 0, right, left)


def full(shape):
    return pl.BlockSpec(shape, lambda *_: (0,) * len(shape))


def some(rows, shape):
    return pl.BlockSpec((rows, *shape), lambda i, *_: (i,) + (0,) * len(shape))


def params(mib):
    return pltpu.CompilerParams(vmem_limit_bytes=mib * 1024 * 1024)


def norm(pair, gain, w_bias, core):
    rows, cols, channels = pair.shape
    half = rows // 2
    return pl.pallas_call(
        norm_kernel,
        grid_spec=pltpu.PrefetchScalarGridSpec(
            num_scalar_prefetch=1,
            grid=(2,),
            in_specs=[
                pl.BlockSpec((half, cols, channels), lambda i, s: (lax.rem(i + s[0], 2), 0, 0)),
                full((1, channels)),
                full((2, channels)),
            ],
            out_specs=[
                full((half, cols, channels)),
                pl.BlockSpec((2, half, cols), lambda i, s: (0, lax.rem(i + s[0], 2), 0)),
            ],
            scratch_shapes=[pltpu.VMEM((2, half, cols), jnp.float32)],
        ),
        out_shape=[
            jax.ShapeDtypeStruct((half, cols, channels), jnp.bfloat16),
            jax.ShapeDtypeStruct((2, rows, cols), jnp.bfloat16),
        ],
        compiler_params=params(NORM_VMEM),
        cost_estimate=pl.CostEstimate(
            flops=4_000_000_000, bytes_accessed=4_000_000, transcendentals=0
        ),
        name="norm",
    )(core[None], pair, gain[None], w_bias.T)


def project(sources, packs):
    half, cols, channels = sources[0].shape
    step = STEP
    second = len(packs) == 2
    row = some(step, (cols, channels))
    shape = jax.ShapeDtypeStruct
    out_specs = [row, row]
    out_shape = [
        shape((half, cols, channels), jnp.bfloat16),
        shape((half, cols, channels), jnp.float32),
    ]
    for blocks in (len(sources), 1) if second else (len(sources),):
        length = blocks * cols
        out_specs += [some(step, (64, length)), some(step, (length, channels))]
        out_shape += [
            shape((half, 64, length), jnp.bfloat16),
            shape((half, length, channels), jnp.bfloat16),
        ]
    return pl.pallas_call(
        project_second if second else project_first,
        grid=(half // step,),
        in_specs=[row] * len(sources) + [full(p.shape) for p in packs],
        out_specs=out_specs,
        out_shape=out_shape,
        compiler_params=params(PROJECT_VMEM),
        cost_estimate=pl.CostEstimate(
            flops=4_000_000_000, bytes_accessed=10_000_000, transcendentals=0
        ),
    )(*sources, *packs)


def attend(scalars, counts, q, g, ks, vs, blocks, phase, groups, before=None, wout=None):
    half, cols, channels = q.shape
    length = groups * cols
    step = STEP
    row = some(step, (cols, channels))
    in_specs = [row, row]
    in_specs += [some(step, a.shape[1:]) for a in (*ks, *vs)]
    in_specs += [full(b.shape) for b in blocks]
    args = [q, g, *ks, *vs, *blocks]
    if phase == 0:
        out_specs = row
        out_shape = jax.ShapeDtypeStruct((half, cols, channels), jnp.bfloat16)
    else:
        in_specs += [row, full(wout.shape)]
        args += [before, wout]
        out_specs = [some(step, (cols // 2, channels))] * 2
        out_shape = [jax.ShapeDtypeStruct((half, cols // 2, channels), jnp.bfloat16)] * 2
    return pl.pallas_call(
        functools.partial(attend_kernel, phase=phase, groups=groups),
        grid_spec=pltpu.PrefetchScalarGridSpec(
            num_scalar_prefetch=2,
            grid=(half // step,),
            in_specs=in_specs,
            out_specs=out_specs,
            scratch_shapes=[
                pltpu.VMEM((2 * cols, length), jnp.float32),
                pltpu.VMEM((2 * cols, length), jnp.float32),
                pltpu.VMEM((2 * cols, length), jnp.float32),
                pltpu.VMEM((2 * cols, 128), jnp.float32),
                pltpu.VMEM((2 * cols, 128), jnp.float32),
                pltpu.VMEM((step * cols, channels), jnp.bfloat16),
            ],
        ),
        out_shape=out_shape,
        compiler_params=params(ATTEND_VMEM),
        cost_estimate=pl.CostEstimate(
            flops=14_000_000_000, bytes_accessed=16_000_000, transcendentals=8_000_000
        ),
    )(scalars, counts, *args)


def per_device(
    pair, seq_length, tile_counts, ln_gain, w_query, w_key, w_value, w_gate, w_bias, w_out
):
    rows, _, _ = pair.shape
    half = rows // 2
    size = lax.axis_size("rows")
    groups = lax.axis_size("keys")
    core = lax.axis_index("heads")
    place = lax.rem(lax.axis_index("rows"), SEGMENT)
    lane_at = lax.axis_index("keys")
    swap = [(0, 1), (1, 0)]

    n0, bias = norm(pair, ln_gain, w_bias, core)

    n1 = lax.ppermute(n0, "keys", shift(groups, 1))
    n2 = lax.ppermute(n0, "keys", shift(groups, -1))

    stride = [[i + SEGMENT * j for j in range(size // SEGMENT)] for i in range(SEGMENT)]
    far = lax.all_gather(bias, "rows", axis=0, axis_index_groups=stride)
    turned = lax.all_to_all(far, "keys", 0, 0, tiled=True)
    down = lax.ppermute(turned, "rows", shift(size, 3))
    up = lax.ppermute(turned, "rows", shift(size, -3))

    blank = jnp.zeros_like(w_query)
    turned_key = jnp.concatenate([w_key.T, blank.T], axis=0)
    mine = jnp.concatenate([w_query, w_query, w_gate, blank, w_value, blank, turned_key], axis=1)
    mine, _ = lax.optimization_barrier((mine, far))
    other = lax.ppermute(mine, "heads", swap)
    late, _ = lax.optimization_barrier((n0, turned))
    n3 = lax.ppermute(late, "keys", shift(groups, 2))

    q0, g0, k0, v0 = project((n0, n1, n2), (mine,))
    down, up, q0 = lax.optimization_barrier((down, up, q0))

    three = jnp.stack([turned, down, up])
    below = lax.ppermute(three, "rows", shift(size, 1))
    above = lax.ppermute(three[:2], "rows", shift(size, -1))
    other, _ = lax.optimization_barrier((other, q0))
    q1, g1, k1, v1, k_late, v_late = project((n0, n1, n2, n3), (mine, other))
    below, above, q1 = lax.optimization_barrier((below, above, q1))
    five = jnp.concatenate([below, above])

    blocks = (three, five)
    three_other = lax.ppermute(three, "heads", swap)
    blocks_other = (three_other, lax.ppermute(five, "heads", swap))

    scalars = jnp.stack([place, lane_at, seq_length[0], core]).astype(jnp.int32)
    counts = lax.dynamic_slice_in_dim(tile_counts, core * half, half, 0).reshape(-1)
    gated = attend(
        scalars, counts, q0, g0, (k0, k_late), (v0, v_late), blocks, 0, groups
    )
    keep, send = attend(
        scalars, counts, q1, g1, (k1,), (v1,), blocks_other, 1, groups, gated, w_out
    )

    got = lax.ppermute(send, "heads", swap)
    return jnp.where(
        core == 0, jnp.concatenate([keep, got], axis=0), jnp.concatenate([got, keep], axis=0)
    )


def solution(mesh):
    in_specs = (
        P(("groups", "rows"), "keys", None),
        P("groups"),
        P(("groups", "rows"), None),
        P(),
        P(None, "heads"),
        P(None, "heads"),
        P(None, "heads"),
        P(None, "heads"),
        P(None, "heads"),
        P(),
    )
    out_specs = P(("groups", "rows"), ("keys", "heads"), None)

    return jax.shard_map(per_device, mesh=mesh, in_specs=in_specs, out_specs=out_specs, check_vma=False)
```
